32 devices in a mesh: pair: 4 (over y, x), aux: 8 (over z, core).
Axes of the slice: x: 2, y: 2, z: 4, core: 2. Of those that a mesh axis runs over, the one named last changes fastest.
Arguments:
- amplitudes: bfloat16 [4, 512, 512], P('pair', 'aux'), may hold values from -6 to 6
- factors: bfloat16 [4096, 512, 512], P('aux', 'pair'), may hold values from -0.03125 to 0.03125
- hole_weights: float32 [4, 4], replicated, may hold values from -3 to 3
- driver: float32 [4, 6, 512], P('pair', None, 'aux'), may hold values from -6 to 6
- eps_vir: float32 [512], replicated, may hold values from 0.5 to 3
- pair_energy: float32 [4], P('pair'), may hold values from -3 to -0.5
Outputs:
- residual: float32 [4, 6, 512], P('pair', None, 'aux')
- new_amps: float32 [4, 6, 512], P('pair', None, 'aux')
The draws below stay inside these ranges and needn't reach their ends.
All inputs are finite; a program needn't handle non-finite values.
Results may differ from the reference program's by a relative error of at most 0.0003.
Values may be sent and summed in bfloat16 or wider, within the bound.
A program may use at most 192 MiB of HBM per device.

```python
import jax
import jax.numpy as jnp
from jax import lax

V = 512
NAUX = 4096
A = 6
P_SIZE = 4


def block_levels(key, extent, pieces, least, largest):
    level, own = 1.0, jax.random.fold_in(key, 6)
    for axis_at, parts in pieces:
        draws = jnp.exp(jax.random.uniform(jax.random.fold_in(own, axis_at), (parts,), jnp.float32, least / len(pieces), largest / len(pieces)))
        level = level * jnp.repeat(draws, extent[axis_at] // parts).reshape([-1 if axis == axis_at else 1 for axis in range(len(extent))])
    return level


def scatter_about(own_key, dims, width, reach, cuts=(), dtype=jnp.bfloat16):
    gain = block_levels(own_key, dims, cuts, -0.22, 0.18) if cuts else 1.0
    entries = jax.random.normal(own_key, dims, jnp.float32) * width * gain
    return jnp.minimum(jnp.maximum(entries, -reach), reach).astype(dtype)


def setup_inputs(seed: int = 0) -> dict:
    key_of = jax.random.split(jax.random.key(seed), 7)
    return {
        "amplitudes": scatter_about(key_of[0], (P_SIZE, V, V), 1.0, 6.0, ((0, 4), (1, 8))),
        "factors": scatter_about(key_of[1], (NAUX, V, V), (V * 64) ** -0.5, 0.03125, ((0, 8), (1, 4))),
        "hole_weights": scatter_about(key_of[2], (P_SIZE, P_SIZE), P_SIZE ** -0.5, 3.0, (), jnp.float32),
        "driver": scatter_about(key_of[3], (P_SIZE, A, V), 1.0, 6.0, ((0, 4), (2, 8)), jnp.float32),
        "eps_vir": jnp.clip(jax.random.uniform(key_of[4], (V,), jnp.float32, 0.5, 3.0), 0.5, 3.0),
        "pair_energy": jnp.clip(-3.0 + 2.5 * jax.random.uniform(key_of[5], (P_SIZE,), jnp.float32) ** block_levels(key_of[5], (P_SIZE,), ((0, 4),), -0.2, 0.2), -3.0, -0.5),
    }


def reference(amplitudes, factors, hole_weights, driver, eps_vir, pair_energy):
    block_size = min(128, NAUX)
    block_count = NAUX // block_size
    amp_wide = amplitudes.astype(jnp.float32)
    stacked = factors.reshape(block_count, block_size, V, V)

    def add_block(total, factor_block):
        wide = factor_block.astype(jnp.float32)
        halves = jnp.einsum("qac,pcd->paqd", wide[:, :A, :], amp_wide, precision=lax.Precision.HIGHEST).astype(jnp.bfloat16)
        term = jnp.einsum("paqd,qbd->pab", halves.astype(jnp.float32), wide, precision=lax.Precision.HIGHEST)
        return total + term, None

    particle, unused = lax.scan(add_block, jnp.zeros((P_SIZE, A, V), jnp.float32), stacked)
    amp_window = amp_wide[:, :A, :]
    hole_term = jnp.einsum("pk,kab->pab", hole_weights, amp_window, precision=lax.Precision.HIGHEST)
    residual = driver + particle + hole_term
    denominator = eps_vir[:A][None, :, None] + eps_vir[None, None, :] - pair_energy[:, None, None]
    new_amps = amp_window - residual / denominator
    return residual, new_amps
```

```python
import functools

import jax
import jax.numpy as jnp
from jax import lax
from jax.experimental import pallas as pl
from jax.experimental.pallas import tpu as pltpu
from jax.sharding import PartitionSpec as P

MESH = pl.DeviceIdType.MESH
F32 = jnp.float32
BF16 = jnp.bfloat16
PAD = 8
SPLIT = 2
LEAD = 2
STAGES = (-2, 1, 2)
PACE = (9, 10)


def ring_order(n):
    side = 1
    while side * side < n:
        side += 1
    if side * side != n or side % 2:
        return list(range(n))
    order = []
    for row in range(side):
        cols = list(range(1, side))
        if row % 2:
            cols.reverse()
        if row == 0:
            cols = [0] + cols
        order += [row * side + col for col in cols]
    order += [row * side for row in range(side - 1, 0, -1)]
    return order


def lookup(index, table):
    value = jnp.int32(table[0])
    for at, entry in enumerate(table[1:], 1):
        value = jnp.where(index == at, jnp.int32(entry), value)
    return value


def kernel(
    n_pair, n_aux, rows, columns, chunk, unit, slots, early,
    amp_ref, fac_ref, hole_ref, driver_ref, eps_ref, eps_row_ref, energy_ref,
    res_ref, new_ref,
    t_ref, w8_ref, w_ref, f_ref, h_ref, part_ref, flip_ref, send_ref, got_ref, keep_ref, pick_ref,
    f_sem, loc_sem, w8_sem, o_send, o_recv, y_send, y_recv, m_send, m_recv,
    z_send, z_recv, c_send, c_recv, w_send, w_recv, r_send, r_recv,
):
    width = amp_ref.shape[2]
    own_rows = amp_ref.shape[1]
    depth, block = fac_ref.shape[:2]
    chunks = depth // chunk
    units = depth // unit
    per = chunk // unit
    steps = units // 2
    m = n_aux // 2
    half = m // 2
    i = lax.axis_index("pair")
    j = lax.axis_index("aux")
    z = j // 2
    core = lax.rem(j, 2)
    mirror = lax.rem(z + half, m)
    base = (z // half) * half
    far = (mirror // half) * half

    order = ring_order(n_pair)
    where = [order.index(k) for k in range(n_pair)]
    pos = lookup(i, where)
    right = lookup(i, [order[(where[k] + 1) % n_pair] for k in range(n_pair)])
    left = lookup(i, [order[(where[k] - 1) % n_pair] for k in range(n_pair)])

    def rows_of(at):
        return pl.ds(pl.multiple_of(at * own_rows, own_rows), own_rows)

    def load_factors(k):
        slot = lax.rem(k, slots)
        return pltpu.make_async_copy(
            fac_ref.at[pl.ds(pl.multiple_of(k * chunk, chunk), chunk)], f_ref.at[slot], f_sem.at[slot]
        )

    def w8_load(k):
        return pltpu.make_async_copy(
            fac_ref.at[pl.ds(pl.multiple_of(k * chunk, chunk), chunk), pl.ds(0, PAD)], w8_ref.at[k], w8_sem.at[k]
        )

    def o_copy(peer, source):
        return pltpu.make_async_remote_copy(
            src_ref=amp_ref.at[0], dst_ref=t_ref.at[source, rows_of(j)],
            send_sem=o_send.at[peer], recv_sem=o_recv.at[source],
            device_id=(peer, j), device_id_type=MESH,
        )

    def mirror_copy(target, source):
        return pltpu.make_async_remote_copy(
            src_ref=amp_ref.at[0], dst_ref=t_ref.at[i, rows_of(source * 2 + core)],
            send_sem=y_send, recv_sem=y_recv,
            device_id=(i, target * 2 + core), device_id_type=MESH,
        )

    def m_copy(peer, source):
        held = rows_of(mirror * 2 + core)
        return pltpu.make_async_remote_copy(
            src_ref=t_ref.at[source, held], dst_ref=t_ref.at[source, held],
            send_sem=m_send.at[peer], recv_sem=m_recv.at[source],
            device_id=(peer, j), device_id_type=MESH,
        )

    def z_copy(target, group):
        held = rows_of(group * 2 + core)
        at = lax.rem(target + half - base, half) + jnp.where(group // half == z // half, 0, half)
        return pltpu.make_async_remote_copy(
            src_ref=t_ref.at[:, held], dst_ref=t_ref.at[:, held],
            send_sem=z_send.at[at], recv_sem=z_recv.at[group],
            device_id=(i, target * 2 + core), device_id_type=MESH,
        )

    def c_copy(group, own):
        held = rows_of(group * 2 + own)
        return pltpu.make_async_remote_copy(
            src_ref=t_ref.at[:, held], dst_ref=t_ref.at[:, held],
            send_sem=c_send.at[group], recv_sem=c_recv.at[group],
            device_id=(i, z * 2 + 1 - core), device_id_type=MESH,
        )

    def w_copy(u, target):
        return pltpu.make_async_remote_copy(
            src_ref=w_ref.at[u], dst_ref=w_ref.at[u],
            send_sem=w_send.at[u], recv_sem=w_recv.at[u],
            device_id=(target, j), device_id_type=MESH,
        )

    targets = (right, left)
    distances = (pos, lax.rem(n_pair - pos, n_pair))

    def squeeze(k):
        w8_load(k).wait()
        wide = w8_ref[k].reshape(chunk * PAD, width)
        tight = jnp.dot(pick_ref[...], wide, preferred_element_type=F32).astype(BF16)
        w_ref[pl.ds(k * per, per)] = tight.reshape(per, unit * rows, width)

    def send_units(k):
        for at in range(per):
            w_copy(k * per + at, targets[at % 2]).start()

    near = jnp.where(distances[0] <= distances[1], 0, 1)

    def distance(d):
        return jnp.where(d == 0, distances[0], distances[1])

    def handle(first, last):
        @pl.when(pos > 0)
        def _():
            for d in (near, 1 - near):
                target = jnp.where(d == 0, right, left)

                @pl.loop(first(d), last(d))
                def _(s):
                    u = 2 * s + d
                    w_copy(u, target).wait_recv()

                    @pl.when(distance(d) < n_pair - 1)
                    def _():
                        w_copy(u, target).start()

    def ready(d, base):
        return jnp.clip(base + LEAD * (n_pair - 1 - distance(d)), 0, steps)

    local = pltpu.make_async_copy(amp_ref.at[0], t_ref.at[i, rows_of(j)], loc_sem)
    local.start()
    mirror_copy(mirror, z).start()
    for step in range(1, n_pair):
        peer = lax.rem(i + step, n_pair)
        o_copy(peer, i).start()

    @pl.when(pos == 0)
    def _():
        for k in range(chunks):
            w8_load(k).start()
        row = lax.broadcasted_iota(jnp.int32, pick_ref.shape, 0)
        col = lax.broadcasted_iota(jnp.int32, pick_ref.shape, 1)
        hit = (row == (col // PAD) * rows + col % PAD) & (col % PAD < rows)
        pick_ref[...] = jnp.where(hit, 1.0, 0.0).astype(BF16)

    for k in range(slots):
        load_factors(k).start()

    @pl.when(pos == 0)
    def _():
        for k in range(early):
            squeeze(k)
        for k in range(early):
            send_units(k)

    local.wait()
    for step in range(1, n_pair):
        source = lax.rem(i + n_pair - step, n_pair)
        o_copy(i, source).wait_recv()
    for step in range(1, half):
        z_copy(base + lax.rem(z - base + step, half), z).start()
    c_copy(z, core).start()

    mirror_copy(z, mirror).wait_recv()
    for step in range(1, n_pair):
        peer = lax.rem(i + step, n_pair)
        m_copy(peer, i).start()

    @pl.when(pos == 0)
    def _():
        squeeze(early)

        @pl.loop(early, chunks)
        def _(k):
            @pl.when(k + 1 < chunks)
            def _():
                squeeze(k + 1)

            send_units(k)

    for step in range(1, n_pair):
        source = lax.rem(i + n_pair - step, n_pair)
        m_copy(i, source).wait_recv()
    for step in range(1, half):
        z_copy(base + lax.rem(z - base + step, half), mirror).start()
    c_copy(mirror, core).start()

    handle(lambda d: 0, lambda d: ready(d, STAGES[0]))
    for step in range(1, half):
        source = base + lax.rem(z - base + half - step, half)
        z_copy(z, source).wait_recv()
        c_copy(source, core).start()
    handle(lambda d: ready(d, STAGES[0]), lambda d: ready(d, STAGES[1]))
    for step in range(1, half):
        source = far + lax.rem(z - base + half - step, half)
        z_copy(z, source).wait_recv()
        c_copy(source, core).start()

    flip_ref[...] = jnp.zeros_like(flip_ref)
    part_ref[...] = jnp.zeros_like(part_ref)
    e_row = lax.broadcasted_iota(jnp.int32, (chunk * PAD, chunk * rows), 0)
    e_col = lax.broadcasted_iota(jnp.int32, (chunk * PAD, chunk * rows), 1)
    hit = (e_col == (e_row // PAD) * rows + e_row % PAD) & (e_row % PAD < rows)
    keep_ref[...] = jnp.where(hit, 1.0, 0.0).astype(BF16)

    for group in range(m):
        c_copy(group, 1 - core).wait_recv()

    def handled(d, k):
        value = jnp.maximum(
            ready(d, STAGES[2] + (k * PACE[0]) // PACE[1]), jnp.minimum((k + 1) * per // 2, steps)
        )
        return jnp.where(k < 0, ready(d, STAGES[1]), value)

    @pl.loop(0, chunks)
    def _(k):
        handle(lambda d: handled(d, k - 1), lambda d: handled(d, k))
        load_factors(k).wait()
        slot = lax.rem(k, slots)
        tight = w_ref[pl.ds(k * per, per)].reshape(chunk * rows, width)
        wide = jnp.dot(keep_ref[...], tight, preferred_element_type=F32).astype(BF16)
        for p in range(0, n_pair, 2):
            two = [
                jnp.dot(wide, t_ref[p + at], preferred_element_type=F32).reshape(chunk, PAD, width)
                for at in range(2)
            ]
            h_ref[:, p * PAD : (p + 2) * PAD, :] = jnp.concatenate(two, axis=1).astype(BF16)

        def add(g, totals):
            flip, part = totals
            flip = flip + lax.dot_general(
                f_ref[slot, 2 * g], h_ref[2 * g], (((1,), (1,)), ((), ())), preferred_element_type=F32
            )
            part = part + lax.dot_general(
                h_ref[2 * g + 1], f_ref[slot, 2 * g + 1], (((1,), (1,)), ((), ())), preferred_element_type=F32
            )
            return flip, part

        zeros = (jnp.zeros((block, n_pair * PAD), F32), jnp.zeros((n_pair * PAD, block), F32))
        flip, part = lax.fori_loop(0, chunk // 2, add, zeros, unroll=chunk // 2)
        flip_ref[...] += flip
        part_ref[...] += part

        @pl.when(k + slots < chunks)
        def _():
            load_factors(k + slots).start()

    send_ref[...] = (flip_ref[...].T + part_ref[...]).reshape(n_pair, PAD, block)
    ratio = n_aux // n_pair

    def r_copy(p, t, source, to):
        return pltpu.make_async_remote_copy(
            src_ref=send_ref.at[p], dst_ref=got_ref.at[source],
            send_sem=r_send.at[p * ratio + t], recv_sem=r_recv.at[source],
            device_id=to, device_id_type=MESH,
        )

    for p in range(n_pair):
        for t in range(ratio):
            column = i * ratio + t
            mine = (i == p) & (j == column)

            @pl.when(mine)
            def _():
                got_ref[j] = send_ref[p]

            @pl.when(jnp.logical_not(mine))
            def _():
                r_copy(p, t, j, (jnp.int32(p), column)).start()

    def cut(values):
        out = values[..., :columns]
        for at in range(1, n_aux):
            out = jnp.where(j == at, values[..., at * columns : (at + 1) * columns], out)
        return out

    hole = jnp.zeros((PAD, columns), F32)
    mine = jnp.zeros((PAD, columns), F32)
    for p in range(n_pair):
        slab = cut(t_ref[p, 0:16, :].astype(F32)[:PAD])
        hole = hole + hole_ref[i, p] * slab
        mine = jnp.where(i == p, slab, mine)
    eps_cols = cut(eps_row_ref[...])
    a_at = lax.broadcasted_iota(jnp.int32, (PAD, columns), 0)
    eps_rows = jnp.zeros((PAD, columns), F32)
    for a in range(rows):
        eps_rows = jnp.where(a_at == a, eps_ref[a], eps_rows)
    denominator = (eps_rows + eps_cols - energy_ref[0])[:rows]
    fixed = driver_ref[0] + hole[:rows]

    column_owner = j // ratio
    for source in range(n_aux):
        @pl.when(jnp.logical_not((column_owner == i) & (j == source)))
        def _():
            r_copy(0, 0, source, (i, j)).wait_recv()

    total = got_ref[0]
    for source in range(1, n_aux):
        total = total + got_ref[source]
    particle = total[:, :columns]
    for t in range(1, ratio):
        particle = jnp.where(lax.rem(j, ratio) == t, total[:, t * columns : (t + 1) * columns], particle)
    residual = fixed + particle[:rows]
    res_ref[0] = residual
    new_ref[0] = mine[:rows] - residual / denominator

    for p in range(n_pair):
        for t in range(ratio):
            column = i * ratio + t

            @pl.when(jnp.logical_not((i == p) & (j == column)))
            def _():
                r_copy(p, t, j, (jnp.int32(p), column)).wait_send()
    mirror_copy(mirror, z).wait_send()
    for step in range(1, n_pair):
        peer = lax.rem(i + step, n_pair)
        o_copy(peer, i).wait_send()
        m_copy(peer, i).wait_send()
    for step in range(1, half):
        target = base + lax.rem(z - base + step, half)
        z_copy(target, z).wait_send()
        z_copy(target, mirror).wait_send()
    for group in range(m):
        c_copy(group, core).wait_send()

    for d in range(2):
        @pl.when(distances[d] < n_pair - 1)
        def _():
            @pl.loop(0, steps)
            def _(s):
                w_copy(2 * s + d, targets[d]).wait_send()


def per_device(n_pair, n_aux, amplitudes, factors, hole_weights, driver, eps_vir, pair_energy):
    rows, columns = driver.shape[1:]
    depth, block, width = factors.shape
    own_rows = amplitudes.shape[1]
    chunk = min(32, depth)
    unit = chunk // SPLIT
    chunks = depth // chunk
    units = depth // unit
    slots = min(8, chunks)
    early = min(1, chunks)
    m = n_aux // 2
    half = m // 2
    ratio = n_aux // n_pair
    vmem = pl.BlockSpec(memory_space=pltpu.VMEM)
    smem = pl.BlockSpec(memory_space=pltpu.SMEM)
    hbm = pl.BlockSpec(memory_space=pl.ANY)
    dma = pltpu.SemaphoreType.DMA
    return pl.pallas_call(
        functools.partial(kernel, n_pair, n_aux, rows, columns, chunk, unit, slots, early),
        out_shape=(
            jax.ShapeDtypeStruct(driver.shape, F32),
            jax.ShapeDtypeStruct(driver.shape, F32),
        ),
        in_specs=[hbm, hbm, smem, vmem, smem, vmem, smem],
        out_specs=(vmem, vmem),
        scratch_shapes=[
            pltpu.VMEM((n_pair, n_aux * own_rows, width), BF16),
            pltpu.VMEM((chunks, chunk, PAD, width), BF16),
            pltpu.VMEM((units, unit * rows, width), BF16),
            pltpu.VMEM((slots, chunk, block, width), BF16),
            pltpu.VMEM((chunk, n_pair * PAD, width), BF16),
            pltpu.VMEM((n_pair * PAD, block), F32),
            pltpu.VMEM((block, n_pair * PAD), F32),
            pltpu.VMEM((n_pair, PAD, block), F32),
            pltpu.VMEM((n_aux, PAD, block), F32),
            pltpu.VMEM((chunk * PAD, chunk * rows), BF16),
            pltpu.VMEM((chunk * rows, chunk * PAD), BF16),
            dma((slots,)),
            dma,
            dma((chunks,)),
            dma((n_pair,)),
            dma((n_pair,)),
            dma,
            dma,
            dma((n_pair,)),
            dma((n_pair,)),
            dma((m,)),
            dma((m,)),
            dma((m,)),
            dma((m,)),
            dma((units,)),
            dma((units,)),
            dma((n_pair * ratio,)),
            dma((n_aux,)),
        ],
        compiler_params=pltpu.CompilerParams(has_side_effects=True, vmem_limit_bytes=60 * 1024 * 1024),
    )(amplitudes, factors, hole_weights, driver, eps_vir, eps_vir.reshape(1, width), pair_energy)


def solution(mesh):
    return jax.shard_map(
        functools.partial(per_device, mesh.shape["pair"], mesh.shape["aux"]),
        mesh=mesh,
        in_specs=(
            P("pair", "aux", None),
            P("aux", "pair", None),
            P(),
            P("pair", None, "aux"),
            P(),
            P("pair"),
        ),
        out_specs=(P("pair", None, "aux"), P("pair", None, "aux")),
        check_vma=False,
    )
```

```python
import functools

import jax
import jax.numpy as jnp
from jax import lax
from jax.experimental import pallas as pl
from jax.experimental.pallas import tpu as pltpu
from jax.sharding import PartitionSpec as P

MESH = pl.DeviceIdType.MESH
F32 = jnp.float32
BF16 = jnp.bfloat16
PAD = 8
SPLIT = 2
LEAD = 3
STAGES = (-2, -1, 0)
PACE = (1, 1)
GRANT = 60 * 1024 * 1024


def ring_order(n):
    side = 1
    while side * side < n:
        side += 1
    if side * side != n or side % 2:
        return list(range(n))
    order = []
    for row in range(side):
        cols = list(range(1, side))
        if row % 2:
            cols.reverse()
        if row == 0:
            cols = [0] + cols
        order += [row * side + col for col in cols]
    order += [row * side for row in range(side - 1, 0, -1)]
    return order


def lookup(index, table):
    value = jnp.int32(table[0])
    for at, entry in enumerate(table[1:], 1):
        value = jnp.where(index == at, jnp.int32(entry), value)
    return value


def kernel(
    n_pair, n_aux, rows, columns, chunk, unit, slots, early,
    amp_ref, fac_ref, hole_ref, driver_ref, eps_ref, eps_row_ref, energy_ref,
    out_ref,
    t_ref, w8_ref, w_ref, f_ref, h_ref, part_ref, flip_ref, send_ref, got_ref, keep_ref, pick_ref, d_ref,
    f_sem, loc_sem, d_sem, w8_sem, o_send, o_recv, y_send, y_recv, m_send, m_recv,
    z_send, z_recv, c_send, c_recv, w_send, w_recv, r_send, r_recv,
):
    width = amp_ref.shape[2]
    own_rows = amp_ref.shape[1]
    depth, block = fac_ref.shape[:2]
    chunks = depth // chunk
    units = depth // unit
    per = chunk // unit
    steps = units // 2
    m = n_aux // 2
    half = m // 2
    i = lax.axis_index("pair")
    j = lax.axis_index("aux")
    z = j // 2
    core = lax.rem(j, 2)
    mirror = lax.rem(z + half, m)
    base = (z // half) * half
    far = (mirror // half) * half

    order = ring_order(n_pair)
    where = [order.index(k) for k in range(n_pair)]
    pos = lookup(i, where)
    right = lookup(i, [order[(where[k] + 1) % n_pair] for k in range(n_pair)])
    left = lookup(i, [order[(where[k] - 1) % n_pair] for k in range(n_pair)])

    def rows_of(at):
        return pl.ds(pl.multiple_of(at * own_rows, own_rows), own_rows)

    def load_factors(k):
        slot = lax.rem(k, slots)
        return pltpu.make_async_copy(
            fac_ref.at[pl.ds(pl.multiple_of(k * chunk, chunk), chunk)], f_ref.at[slot], f_sem.at[slot]
        )

    def w8_load(k):
        return pltpu.make_async_copy(
            fac_ref.at[pl.ds(pl.multiple_of(k * chunk, chunk), chunk), pl.ds(0, PAD)], w8_ref.at[k], w8_sem.at[k]
        )

    def o_copy(peer, source):
        return pltpu.make_async_remote_copy(
            src_ref=amp_ref.at[0], dst_ref=t_ref.at[source, rows_of(j)],
            send_sem=o_send.at[peer], recv_sem=o_recv.at[source],
            device_id=(peer, j), device_id_type=MESH,
        )

    def mirror_copy(target, source):
        return pltpu.make_async_remote_copy(
            src_ref=amp_ref.at[0], dst_ref=t_ref.at[i, rows_of(source * 2 + core)],
            send_sem=y_send, recv_sem=y_recv,
            device_id=(i, target * 2 + core), device_id_type=MESH,
        )

    def m_copy(peer, source):
        held = rows_of(mirror * 2 + core)
        return pltpu.make_async_remote_copy(
            src_ref=t_ref.at[source, held], dst_ref=t_ref.at[source, held],
            send_sem=m_send.at[peer], recv_sem=m_recv.at[source],
            device_id=(peer, j), device_id_type=MESH,
        )

    def z_copy(target, group):
        held = rows_of(group * 2 + core)
        at = lax.rem(target + half - base, half) + jnp.where(group // half == z // half, 0, half)
        return pltpu.make_async_remote_copy(
            src_ref=t_ref.at[:, held], dst_ref=t_ref.at[:, held],
            send_sem=z_send.at[at], recv_sem=z_recv.at[group],
            device_id=(i, target * 2 + core), device_id_type=MESH,
        )

    def c_copy(group, own):
        held = rows_of(group * 2 + own)
        return pltpu.make_async_remote_copy(
            src_ref=t_ref.at[:, held], dst_ref=t_ref.at[:, held],
            send_sem=c_send.at[group], recv_sem=c_recv.at[group],
            device_id=(i, z * 2 + 1 - core), device_id_type=MESH,
        )

    def w_copy(u, target):
        return pltpu.make_async_remote_copy(
            src_ref=w_ref.at[u], dst_ref=w_ref.at[u],
            send_sem=w_send.at[u], recv_sem=w_recv.at[u],
            device_id=(target, j), device_id_type=MESH,
        )

    targets = (right, left)
    distances = (pos, lax.rem(n_pair - pos, n_pair))

    def squeeze(k):
        w8_load(k).wait()
        wide = w8_ref[k].reshape(chunk * PAD, width)
        tight = jnp.dot(pick_ref[...], wide, preferred_element_type=F32).astype(BF16)
        w_ref[pl.ds(k * per, per)] = tight.reshape(per, unit * rows, width)

    def send_units(k):
        for at in range(per):
            w_copy(k * per + at, targets[at % 2]).start()

    near = jnp.where(distances[0] <= distances[1], 0, 1)

    def distance(d):
        return jnp.where(d == 0, distances[0], distances[1])

    def handle(first, last):
        @pl.when(pos > 0)
        def _():
            for d in (near, 1 - near):
                target = jnp.where(d == 0, right, left)

                @pl.loop(first(d), last(d))
                def _(s):
                    u = 2 * s + d
                    w_copy(u, target).wait_recv()

                    @pl.when(distance(d) < n_pair - 1)
                    def _():
                        w_copy(u, target).start()

    def ready(d, base):
        return jnp.clip(base + LEAD * (n_pair - 1 - distance(d)), 0, steps)

    local = pltpu.make_async_copy(amp_ref.at[0], t_ref.at[i, rows_of(j)], loc_sem)
    local.start()
    driver_load = pltpu.make_async_copy(driver_ref, d_ref, d_sem)
    driver_load.start()

    @pl.when(pos == 0)
    def _():
        for k in range(chunks):
            w8_load(k).start()

    barrier = pltpu.get_barrier_semaphore()
    friends = [(lax.rem(i + step, n_pair), j) for step in range(1, n_pair)]
    friends += [(i, (base + lax.rem(z - base + step, half)) * 2 + core) for step in range(1, half)]
    friends += [(i, mirror * 2 + core), (i, z * 2 + 1 - core)]
    for friend in friends:
        pl.semaphore_signal(barrier, inc=1, device_id=friend, device_id_type=MESH)

    @pl.when(pos == 0)
    def _():
        row = lax.broadcasted_iota(jnp.int32, pick_ref.shape, 0)
        col = lax.broadcasted_iota(jnp.int32, pick_ref.shape, 1)
        hit = (row == (col // PAD) * rows + col % PAD) & (col % PAD < rows)
        pick_ref[...] = jnp.where(hit, 1.0, 0.0).astype(BF16)
        for k in range(early):
            squeeze(k)

    pl.semaphore_wait(barrier, len(friends))

    mirror_copy(mirror, z).start()
    for step in range(1, n_pair):
        peer = lax.rem(i + step, n_pair)
        o_copy(peer, i).start()


    @pl.when(pos == 0)
    def _():
        for k in range(early):
            send_units(k)

    for k in range(slots):
        load_factors(k).start()

    local.wait()
    for step in range(1, n_pair):
        source = lax.rem(i + n_pair - step, n_pair)
        o_copy(i, source).wait_recv()
    for step in range(1, half):
        z_copy(base + lax.rem(z - base + step, half), z).start()
    c_copy(z, core).start()

    mirror_copy(z, mirror).wait_recv()
    for step in range(1, n_pair):
        peer = lax.rem(i + step, n_pair)
        m_copy(peer, i).start()

    @pl.when(pos == 0)
    def _():
        squeeze(early)

        @pl.loop(early, chunks)
        def _(k):
            @pl.when(k + 1 < chunks)
            def _():
                squeeze(k + 1)

            send_units(k)

    for step in range(1, n_pair):
        source = lax.rem(i + n_pair - step, n_pair)
        m_copy(i, source).wait_recv()
    for step in range(1, half):
        z_copy(base + lax.rem(z - base + step, half), mirror).start()
    c_copy(mirror, core).start()

    handle(lambda d: 0, lambda d: ready(d, STAGES[0]))
    for step in range(1, half):
        source = base + lax.rem(z - base + half - step, half)
        z_copy(z, source).wait_recv()
        c_copy(source, core).start()
    handle(lambda d: ready(d, STAGES[0]), lambda d: ready(d, STAGES[1]))
    for step in range(1, half):
        source = far + lax.rem(z - base + half - step, half)
        z_copy(z, source).wait_recv()
        c_copy(source, core).start()

    flip_ref[...] = jnp.zeros_like(flip_ref)
    part_ref[...] = jnp.zeros_like(part_ref)
    e_row = lax.broadcasted_iota(jnp.int32, (chunk * PAD, chunk * rows), 0)
    e_col = lax.broadcasted_iota(jnp.int32, (chunk * PAD, chunk * rows), 1)
    hit = (e_col == (e_row // PAD) * rows + e_row % PAD) & (e_row % PAD < rows)
    keep_ref[...] = jnp.where(hit, 1.0, 0.0).astype(BF16)

    for group in range(m):
        c_copy(group, 1 - core).wait_recv()

    def handled(d, k):
        value = jnp.maximum(
            ready(d, STAGES[2] + (k * PACE[0]) // PACE[1]), jnp.minimum((k + 1) * per // 2, steps)
        )
        return jnp.where(k < 0, ready(d, STAGES[1]), value)

    @pl.loop(0, chunks)
    def _(k):
        handle(lambda d: handled(d, k - 1), lambda d: handled(d, k))
        load_factors(k).wait()
        slot = lax.rem(k, slots)
        tight = w_ref[pl.ds(k * per, per)].reshape(chunk * rows, width)
        wide = jnp.dot(keep_ref[...], tight, preferred_element_type=F32).astype(BF16)
        for p in range(0, n_pair, 2):
            two = [
                jnp.dot(wide, t_ref[p + at], preferred_element_type=F32).reshape(chunk, PAD, width)
                for at in range(2)
            ]
            h_ref[:, p * PAD : (p + 2) * PAD, :] = jnp.concatenate(two, axis=1).astype(BF16)

        def add(g, totals):
            flip, part = totals
            flip = flip + lax.dot_general(
                f_ref[slot, 2 * g], h_ref[2 * g], (((1,), (1,)), ((), ())), preferred_element_type=F32
            )
            part = part + lax.dot_general(
                h_ref[2 * g + 1], f_ref[slot, 2 * g + 1], (((1,), (1,)), ((), ())), preferred_element_type=F32
            )
            return flip, part

        zeros = (jnp.zeros((block, n_pair * PAD), F32), jnp.zeros((n_pair * PAD, block), F32))
        flip, part = lax.fori_loop(0, chunk // 2, add, zeros, unroll=chunk // 2)
        flip_ref[...] += flip
        part_ref[...] += part

        @pl.when(k + slots < chunks)
        def _():
            load_factors(k + slots).start()

    send_ref[...] = (flip_ref[...].T + part_ref[...]).reshape(n_pair, PAD, block)
    ratio = n_aux // n_pair

    def r_copy(p, t, source, to):
        return pltpu.make_async_remote_copy(
            src_ref=send_ref.at[p], dst_ref=got_ref.at[source],
            send_sem=r_send.at[p * ratio + t], recv_sem=r_recv.at[source],
            device_id=to, device_id_type=MESH,
        )

    for p in range(n_pair):
        for t in range(ratio):
            column = i * ratio + t
            mine = (i == p) & (j == column)

            @pl.when(mine)
            def _():
                got_ref[j] = send_ref[p]

            @pl.when(jnp.logical_not(mine))
            def _():
                r_copy(p, t, j, (jnp.int32(p), column)).start()

    def cut(values):
        out = values[..., :columns]
        for at in range(1, n_aux):
            out = jnp.where(j == at, values[..., at * columns : (at + 1) * columns], out)
        return out

    hole = jnp.zeros((PAD, columns), F32)
    mine = jnp.zeros((PAD, columns), F32)
    for p in range(n_pair):
        slab = cut(t_ref[p, 0:16, :].astype(F32)[:PAD])
        hole = hole + hole_ref[i, p] * slab
        mine = jnp.where(i == p, slab, mine)
    eps_cols = cut(eps_row_ref[...])
    a_at = lax.broadcasted_iota(jnp.int32, (PAD, columns), 0)
    eps_rows = jnp.zeros((PAD, columns), F32)
    for a in range(rows):
        eps_rows = jnp.where(a_at == a, eps_ref[a], eps_rows)
    denominator = (eps_rows + eps_cols - energy_ref[0])[:rows]
    driver_load.wait()
    fixed = jnp.concatenate([d_ref[a] for a in range(rows)], axis=0) + hole[:rows]

    column_owner = j // ratio
    for source in range(n_aux):
        @pl.when(jnp.logical_not((column_owner == i) & (j == source)))
        def _():
            r_copy(0, 0, source, (i, j)).wait_recv()

    total = got_ref[0]
    for source in range(1, n_aux):
        total = total + got_ref[source]
    particle = total[:, :columns]
    for t in range(1, ratio):
        particle = jnp.where(lax.rem(j, ratio) == t, total[:, t * columns : (t + 1) * columns], particle)
    residual = fixed + particle[:rows]
    updated = mine[:rows] - residual / denominator
    for a in range(rows):
        out_ref[a] = residual[a : a + 1]
        out_ref[rows + a] = updated[a : a + 1]

    for p in range(n_pair):
        for t in range(ratio):
            column = i * ratio + t

            @pl.when(jnp.logical_not((i == p) & (j == column)))
            def _():
                r_copy(p, t, j, (jnp.int32(p), column)).wait_send()
    mirror_copy(mirror, z).wait_send()
    for step in range(1, n_pair):
        peer = lax.rem(i + step, n_pair)
        o_copy(peer, i).wait_send()
        m_copy(peer, i).wait_send()
    for step in range(1, half):
        target = base + lax.rem(z - base + step, half)
        z_copy(target, z).wait_send()
        z_copy(target, mirror).wait_send()
    for group in range(m):
        c_copy(group, core).wait_send()

    for d in range(2):
        @pl.when(distances[d] < n_pair - 1)
        def _():
            @pl.loop(0, steps)
            def _(s):
                w_copy(2 * s + d, targets[d]).wait_send()


def per_device(n_pair, n_aux, amplitudes, factors, hole_weights, driver, eps_vir, pair_energy):
    rows, columns = driver.shape[1:]
    depth, block, width = factors.shape
    own_rows = amplitudes.shape[1]
    chunk = min(32, depth)
    unit = chunk // SPLIT
    chunks = depth // chunk
    units = depth // unit
    slots = min(8, chunks)
    early = min(1, chunks)
    m = n_aux // 2
    half = m // 2
    ratio = n_aux // n_pair
    vmem = pl.BlockSpec(memory_space=pltpu.VMEM)
    smem = pl.BlockSpec(memory_space=pltpu.SMEM)
    hbm = pl.BlockSpec(memory_space=pl.ANY)
    dma = pltpu.SemaphoreType.DMA
    out = pl.pallas_call(
        functools.partial(kernel, n_pair, n_aux, rows, columns, chunk, unit, slots, early),
        out_shape=jax.ShapeDtypeStruct((2 * rows, 1, columns), F32),
        in_specs=[hbm, hbm, smem, hbm, smem, vmem, smem],
        out_specs=vmem,
        scratch_shapes=[
            pltpu.VMEM((n_pair, n_aux * own_rows, width), BF16),
            pltpu.VMEM((chunks, chunk, PAD, width), BF16),
            pltpu.VMEM((units, unit * rows, width), BF16),
            pltpu.VMEM((slots, chunk, block, width), BF16),
            pltpu.VMEM((chunk, n_pair * PAD, width), BF16),
            pltpu.VMEM((n_pair * PAD, block), F32),
            pltpu.VMEM((block, n_pair * PAD), F32),
            pltpu.VMEM((n_pair, PAD, block), F32),
            pltpu.VMEM((n_aux, PAD, block), F32),
            pltpu.VMEM((chunk * PAD, chunk * rows), BF16),
            pltpu.VMEM((chunk * rows, chunk * PAD), BF16),
            pltpu.VMEM((rows, 1, columns), F32),
            dma((slots,)),
            dma,
            dma,
            dma((chunks,)),
            dma((n_pair,)),
            dma((n_pair,)),
            dma,
            dma,
            dma((n_pair,)),
            dma((n_pair,)),
            dma((m,)),
            dma((m,)),
            dma((m,)),
            dma((m,)),
            dma((units,)),
            dma((units,)),
            dma((n_pair * ratio,)),
            dma((n_aux,)),
        ],
        compiler_params=pltpu.CompilerParams(collective_id=0, has_side_effects=True, vmem_limit_bytes=GRANT),
    )(
        amplitudes, factors, hole_weights, jnp.swapaxes(driver, 0, 1),
        eps_vir, eps_vir.reshape(1, width), pair_energy,
    )
    return jnp.swapaxes(out[:rows], 0, 1), jnp.swapaxes(out[rows:], 0, 1)


def solution(mesh):
    return jax.shard_map(
        functools.partial(per_device, mesh.shape["pair"], mesh.shape["aux"]),
        mesh=mesh,
        in_specs=(
            P("pair", "aux", None),
            P("aux", "pair", None),
            P(),
            P("pair", None, "aux"),
            P(),
            P("pair"),
        ),
        out_specs=(P("pair", None, "aux"), P("pair", None, "aux")),
        check_vma=False,
    )
```
